32 devices in a mesh: dp: 4 (over x, core), half: 2 (over y), own: 4 (over z).
Axes of the slice: x: 2, y: 2, z: 4, core: 2. Of those that a mesh axis runs over, the one named last changes fastest.
Arguments:
- grad_parts: bfloat16 [4, 6, 1024, 1024], P('dp', None, ('half', 'own')), may hold values from -6 to 6
- owner_table: int32 [6, 1], replicated, may hold values from 0 to 3; in each aligned block of 6 rows (0 to 5, 6 to 11, ...) at most 2 rows name the same one
- left_basis: bfloat16 [8, 1024, 1024], P(('half', 'own')), may hold values from -0.1875 to 0.1875
- right_basis: bfloat16 [8, 1024, 1024], P(('half', 'own')), may hold values from -0.1875 to 0.1875
- first_moment: bfloat16 [8, 1024, 1024], P(('half', 'own'), 'dp'), may hold values from -6 to 6
- second_moment: bfloat16 [8, 1024, 1024], P(('half', 'own'), 'dp'), may hold values from 0.5 to 8
Outputs:
- update: bfloat16 [6, 1024, 1024], P(None, ('half', 'own'), 'dp')
The draws below stay inside these ranges and needn't reach their ends.
Inputs may be any that keep to these rules, and one draw needn't show every extreme that they name: `owner_table`: every owner index is named by at least one block and by at most 2 blocks; some owner is named by exactly 2 blocks.
All inputs are finite; a program needn't handle non-finite values.
Results may differ from the reference program's by a relative error of at most 0.013.
Values may be sent and summed in bfloat16 or wider, within the bound.
A program may use at most 128 MiB of HBM per device.

```python
import math
import jax
import jax.numpy as jnp
import numpy as np
from jax import lax

B = 1024
BLOCKS = 6
SLOTS = 8
N_DP = 4
N_HALF = 2
N_OWN = 4


def block_scale(rng, extent, shards, least, largest):
    def one(axis_at, parts):
        draws = jax.random.uniform(jax.random.fold_in(jax.random.fold_in(rng, 6), axis_at), (parts,), jnp.float32, least / len(shards), largest / len(shards))
        return jnp.repeat(jnp.exp(draws), extent[axis_at] // parts).reshape((-1,) + (1,) * (len(extent) - axis_at - 1))

    factor_of = one(*shards[0])
    for cut in shards[1:]:
        factor_of = factor_of * one(*cut)
    return factor_of


def shared_out(rng, own, number, rows, amount, top, limit, slope):
    sequence = jax.random.permutation(rng, amount)
    heavy_load, ordinary = shares(amount, rows * top, limit, slope, True), shares(amount, rows * top, limit, slope, False)
    places = jnp.arange(amount)

    def named(sizes, offset_by):
        used = int((sizes > 0).sum())
        fixed = max(1, used // 4)
        passed = fixed + (places - fixed + offset_by * (used - fixed)) % max(1, amount - fixed)
        return jnp.zeros((amount,), jnp.int32).at[sequence[jnp.where(places < fixed, places, passed)]].set(jnp.asarray(sizes, jnp.int32))

    sizes = jnp.where(number % 4 == 0, named(heavy_load, number // 4), named(ordinary, number - number // 4 - 1))
    mixed = jax.random.permutation(jax.random.fold_in(own, 3), amount)
    donor, sink = mixed[0:amount // 2 * 2:2], mixed[1:amount // 2 * 2:2]
    margin = jnp.minimum(sizes[donor] - 1, limit - sizes[sink]) // 2
    margin = jnp.where((donor == sequence[0]) | (sink == sequence[0]) | (sizes[sink] == 0), 0, jnp.maximum(margin, 0))
    passed = jax.random.randint(jax.random.fold_in(own, 4), (amount // 2,), 0, 1 << 20) % (margin + 1)
    sizes = sizes.at[donor].add(-passed).at[sink].add(passed)
    items = jnp.searchsorted(jnp.cumsum(sizes), jnp.arange(rows * top), side="right").astype(jnp.int32)
    grid = items.reshape(top, rows).T
    grid = grid[jax.random.permutation(jax.random.fold_in(own, 1), rows)]
    offset_by = jax.random.randint(jax.random.fold_in(own, 2), (rows, 1), 0, top)
    return jnp.take_along_axis(grid, (jnp.arange(top)[None, :] + offset_by) % top, axis=1)


def shares(count, total, reach, lean, full):
    portions = [(1 << 20) // math.isqrt(grade ** lean) + 1 for grade in range(1, count + 1)]
    largest = reach if full else min(reach, max(-(-total // count), total * portions[0] // sum(portions)))
    least = 1 if total - largest >= count - 1 else 0
    holding, surplus = [largest] + [least] * (count - 1), total - largest - least * (count - 1)
    while surplus > 0:
        candidates = [i for i in range(1, count) if holding[i] < largest] or [i for i in range(1, count) if holding[i] < reach]
        pool, budget = sum([portions[i] for i in candidates]), surplus
        for i in candidates:
            extra = min(reach - holding[i], max(1, budget * portions[i] // pool), surplus)
            holding[i] = holding[i] + extra
            surplus = surplus - extra
    return np.array(holding)


def centred(rng, extent, spread, limit, pieces=(), kind=jnp.bfloat16):
    values = jax.random.normal(rng, extent, jnp.float32) * spread
    if len(pieces) > 0:
        values = block_scale(rng, extent, pieces, -0.22, 0.18) * values
    return jnp.clip(values, min=-limit, max=limit).astype(kind)


def setup_inputs(seed: int = 0) -> dict:
    arg_keys = jax.random.split(jax.random.key(seed), 7)
    grad_parts = centred(arg_keys[0], (N_DP, BLOCKS, B, B), 1.0, 6.0, ((0, 4), (2, 8)))
    owner_table_keys = jax.random.split(jax.random.fold_in(arg_keys[1], 1), BLOCKS // BLOCKS)
    owner_table_turns = jax.random.permutation(jax.random.fold_in(arg_keys[1], 3), BLOCKS // BLOCKS)
    owner_table = jax.vmap(lambda own, number: shared_out(jax.random.fold_in(arg_keys[1], 2), own, number, BLOCKS, N_OWN, 1, N_HALF, 2))(owner_table_keys, owner_table_turns).reshape((BLOCKS, 1))
    left_basis = centred(arg_keys[2], (SLOTS, B, B), B ** -0.5, 0.1875, ((0, 8),))
    right_basis = centred(arg_keys[3], (SLOTS, B, B), B ** -0.5, 0.1875, ((0, 8),))
    first_moment = centred(arg_keys[4], (SLOTS, B, B), 1.0, 6.0, ((0, 8), (1, 4)))
    second_moment = jnp.clip(jnp.exp(math.log(8.0) - 2.7725887 * jax.random.uniform(arg_keys[5], (SLOTS, B, B), jnp.float32) ** block_scale(arg_keys[5], (SLOTS, B, B), ((0, 8), (1, 4)), -0.2, 0.2)), 0.5, 8.0).astype(jnp.bfloat16)
    return dict(grad_parts=grad_parts, owner_table=owner_table, left_basis=left_basis, right_basis=right_basis, first_moment=first_moment, second_moment=second_moment)


beta_first = 0.9
beta_second = 0.95
bias_first = 1.0 - 0.9 ** 10
bias_second = 1.0 - 0.95 ** 10
epsilon = 1e-08

def slot_numbers(owner_table):
    owner_ids = owner_table[:, 0].astype(jnp.int32)
    positions = jnp.arange(owner_ids.shape[0], dtype=jnp.int32)
    shared = (owner_ids[:, None] == owner_ids[None, :]) & (positions[None, :] < positions[:, None])
    ranking = lax.optimization_barrier(jnp.sum(shared.astype(jnp.int32), axis=1)).astype(jnp.int32)
    return (ranking * N_OWN + owner_ids).astype(jnp.int32)

def reference(grad_parts, owner_table, left_basis, right_basis, first_moment, second_moment):
    running = grad_parts[0].astype(jnp.float32)
    for replica in range(1, N_DP):
        running = running + grad_parts[replica].astype(jnp.float32)
    gradient = running.astype(jnp.bfloat16)
    slot_ids = slot_numbers(owner_table)

    def per_block(inputs):
        block_grad, slot_index = inputs
        left_matrix = left_basis[slot_index]
        right_matrix = right_basis[slot_index]
        projected = jnp.dot(left_matrix.T, block_grad, preferred_element_type=jnp.float32).astype(jnp.bfloat16)
        rotated = jnp.dot(projected, right_matrix, preferred_element_type=jnp.float32)
        first_new = beta_first * first_moment[slot_index].astype(jnp.float32) + (1.0 - beta_first) * rotated
        second_new = beta_second * second_moment[slot_index].astype(jnp.float32) + (1.0 - beta_second) * rotated * rotated
        direction = (first_new / bias_first / (jnp.sqrt(second_new / bias_second) + epsilon)).astype(jnp.bfloat16)
        back = jnp.dot(direction, right_matrix.T, preferred_element_type=jnp.float32).astype(jnp.bfloat16)
        update = jnp.dot(left_matrix, back, preferred_element_type=jnp.float32)
        return update.astype(jnp.bfloat16)
    return lax.map(per_block, (gradient, slot_ids))
```

```python
import functools

import jax
import jax.numpy as jnp
from jax import lax
from jax.experimental import pallas as pl
from jax.experimental.pallas import tpu as pltpu
from jax.sharding import PartitionSpec as P

beta_first = 0.9
beta_second = 0.95
bias_first = 1.0 - 0.9**10
bias_second = 1.0 - 0.95**10
epsilon = 1e-08


def slot_select(owner_table, owner_count, slot_count):
    owner_ids = owner_table[:, 0]
    positions = jnp.arange(owner_ids.shape[0], dtype=jnp.int32)
    shared = (owner_ids[:, None] == owner_ids[None, :]) & (positions[None, :] < positions[:, None])
    ranking = jnp.sum(shared.astype(jnp.int32), axis=1)
    slot_ids = ranking * owner_count + owner_ids
    slot_range = jnp.arange(slot_count, dtype=jnp.int32)
    return (slot_range[:, None] == slot_ids[None, :]).astype(jnp.bfloat16)


def local(grad_parts, owner_table, left_basis, right_basis, first_moment, second_moment):
    halves = lax.axis_size("half")
    owners = lax.axis_size("own")
    replicas = lax.axis_size("dp")
    block_count = grad_parts.shape[1]
    piece_rows = grad_parts.shape[2]
    block_width = grad_parts.shape[3]
    quarter = block_width // replicas
    offset = lax.axis_index("dp") * quarter
    summed = lax.psum_scatter(
        grad_parts[0].astype(jnp.float32).astype(jnp.bfloat16),
        "dp",
        scatter_dimension=2,
        tiled=True,
    )
    selector = slot_select(owner_table, owners, halves * owners)
    flat_grad = summed.reshape(block_count, piece_rows * quarter)
    packed = jnp.dot(selector, flat_grad, preferred_element_type=jnp.float32).astype(jnp.bfloat16)
    packed = packed.reshape(halves, owners, piece_rows, quarter)
    arrived = lax.all_to_all(
        lax.all_to_all(packed, "half", split_axis=0, concat_axis=0, tiled=True),
        "own",
        split_axis=1,
        concat_axis=1,
        tiled=True,
    )
    grad_block = arrived.reshape(block_width, quarter)
    left_matrix = left_basis[0]
    right_matrix = right_basis[0]
    right_rows = lax.dynamic_slice_in_dim(right_matrix, offset, quarter, 0)
    left_slice = lax.dynamic_slice_in_dim(left_matrix, offset, quarter, 1)
    projected = lax.dot_general(
        left_slice,
        lax.all_gather(grad_block, "dp", axis=1, tiled=True),
        (((0,), (0,)), ((), ())),
        preferred_element_type=jnp.float32,
    )
    rotated = jnp.dot(
        projected.astype(jnp.bfloat16), right_matrix, preferred_element_type=jnp.float32
    )
    first_new = beta_first * first_moment[0].astype(jnp.float32) + (1.0 - beta_first) * rotated
    second_new = (
        beta_second * second_moment[0].astype(jnp.float32) + (1.0 - beta_second) * rotated * rotated
    )
    direction = (first_new / bias_first / (jnp.sqrt(second_new / bias_second) + epsilon)).astype(
        jnp.bfloat16
    )
    partial_cols = lax.dot_general(
        lax.all_gather(direction, "dp", axis=0, tiled=True),
        right_rows,
        (((1,), (1,)), ((), ())),
        preferred_element_type=jnp.float32,
    )
    update_block = jnp.dot(
        left_matrix, partial_cols.astype(jnp.bfloat16), preferred_element_type=jnp.float32
    )
    outgoing = update_block.astype(jnp.bfloat16).reshape(halves, owners, piece_rows, quarter)
    returned = lax.all_to_all(
        lax.all_to_all(outgoing, "half", split_axis=0, concat_axis=0, tiled=True),
        "own",
        split_axis=1,
        concat_axis=1,
        tiled=True,
    )
    flat_back = returned.reshape(halves * owners, piece_rows * quarter)
    placed = lax.dot_general(
        selector, flat_back, (((0,), (0,)), ((), ())), preferred_element_type=jnp.float32
    )
    return placed.astype(jnp.bfloat16).reshape(block_count, piece_rows, quarter)


MESH = pl.DeviceIdType.MESH
LANES = 128
TILE_ROWS = 16
SLOT_CUTS = (1, 1, 2, 2, 2)
PROJ_CUTS = (4, 2, 2)
BACK_CUTS = (1, 1, 2, 4)


def pick(index, values):
    chosen = values[0]
    for i in range(1, len(values)):
        chosen = lax.select_n(index == i, chosen, values[i])
    return chosen


def step_kernel(
    sizes,
    table,
    grad,
    left_in,
    right_in,
    first_in,
    second_in,
    out,
    raw,
    near,
    paired,
    far_in,
    packed,
    grad_turned,
    left,
    right,
    first,
    second,
    first_part,
    second_part,
    proj_out,
    proj_in,
    partial,
    direction,
    back_out,
    back_in,
    update,
    returned,
    chosen,
    raw_sem,
    load_sem,
    near_sem,
    far_sem,
    slot_sem,
    proj_sem,
    back_sem,
    return_sem,
):
    replicas, halves, owners, blocks, rows, width, slot_cuts, proj_cuts, back_cuts = sizes
    far = replicas // 2
    group = halves * owners
    quarter = width // replicas
    lanes = quarter // LANES
    me_dp = lax.axis_index("dp")
    me_group = lax.axis_index("half") * owners + lax.axis_index("own")
    me_far = me_dp // 2
    parity = me_dp % 2
    mate = me_far * 2 + 1 - parity

    middle = max(1, owners // 2)
    sides = owners // middle
    me_half, me_own = me_group // owners, me_group % owners
    side = me_own // middle
    tiles = []
    for across in range(sides - 1, -1, -1):
        for h in range(halves - 1, -1, -1):
            tiles.append(((me_half + h) % halves, (side + across) % sides, across, h))
    others = []
    for h_at, side_at, across, h in tiles:
        for i in range(middle - 1, -1, -1):
            if across or h or i:
                others.append(h_at * owners + side_at * middle + (me_own + i) % middle)

    partners = []
    for j in range(1, far):
        for c in range(2):
            partners.append(((me_far + j) % far) * 2 + (parity + c) % 2)
    partners.append(mate)

    def dp_id(index):
        return {"dp": index}

    def group_id(index):
        return {"half": index // owners, "own": index % owners}

    def remote(src, dst, sems, index, target):
        return pltpu.make_async_remote_copy(
            src_ref=src,
            dst_ref=dst,
            send_sem=sems.at[0],
            recv_sem=sems.at[1 + index],
            device_id=target,
            device_id_type=MESH,
        )

    def received(ref, sems, index):
        remote(ref, ref, sems, index, dp_id(mate)).wait_recv()

    def sent(ref, sems):
        remote(ref, ref, sems, 0, dp_id(mate)).wait_send()

    def span(start, size):
        return slice(start, start + size)

    def index_of(cuts, at):
        return [start <= at < start + size for start, size in cuts].index(True)

    order = list(range(1, far)) + [0]
    raw_loads = {}
    for j in order:
        for k in range(lanes):
            for s in (1, 0):
                index = ((me_far + j) % far) * 2 + (1 - parity if s else parity)
                start = pl.multiple_of(index * quarter + k * LANES, LANES)
                raw_loads[s, j, k] = pltpu.make_async_copy(
                    grad.at[:, :, pl.ds(start, LANES)], raw.at[s, j, k], raw_sem.at[s, j, k]
                )
                raw_loads[s, j, k].start()

    barrier = pltpu.get_barrier_semaphore()
    for j in range(1, replicas):
        pl.semaphore_signal(
            barrier, inc=1, device_id=dp_id((me_dp + j) % replicas), device_id_type=MESH
        )
    for t in range(1, group):
        pl.semaphore_signal(
            barrier, inc=1, device_id=group_id((me_group + t) % group), device_id_type=MESH
        )

    pl.semaphore_wait(barrier, replicas - 1 + group - 1)

    for j in order:
        for k in range(lanes):
            raw_loads[1, j, k].wait()
            remote(
                raw.at[1, j, k], near.at[j, k], near_sem, j * lanes + k, dp_id(mate)
            ).start()

    loads = [
        pltpu.make_async_copy(first_in.at[0], first, load_sem.at[0]),
        pltpu.make_async_copy(second_in.at[0], second, load_sem.at[1]),
        pltpu.make_async_copy(right_in.at[0], right, load_sem.at[2]),
    ]
    left_loads = [
        pltpu.make_async_copy(
            left_in.at[0, :, span(e * quarter, quarter)], left.at[e], load_sem.at[3]
        )
        for e in range(replicas)
    ]
    for load in left_loads + loads:
        load.start()

    for j in order:
        for k in range(lanes):
            raw_loads[0, j, k].wait()
            received(near.at[j, k], near_sem, j * lanes + k)
            for b in range(blocks):
                paired[j, b, span(k * LANES, LANES)] = (
                    (raw[0, j, k, b].astype(jnp.float32) + near[j, k, b].astype(jnp.float32))
                    .astype(jnp.bfloat16)
                    .T
                )
            if j == 0:
                continue
            for i, (start, size) in enumerate(slot_cuts):
                if k * LANES < start + size <= (k + 1) * LANES:
                    remote(
                        paired.at[j, :, span(start, size)],
                        far_in.at[j - 1, :, span(start, size)],
                        far_sem,
                        i,
                        dp_id(((me_far + j) % far) * 2 + parity),
                    ).start()

    def slot_of(b):
        owner = table[b]
        rank = lax.fori_loop(
            0, b, lambda c, n: n + jnp.where(table[c] == owner, 1, 0), jnp.int32(0)
        )
        return rank * owners + owner

    slots = [slot_of(b) for b in range(blocks)]
    block_of = []
    for s in range(group):
        found = jnp.int32(0)
        for b in range(blocks):
            found = jnp.where(slots[b] == s, jnp.int32(b), found)
        block_of.append(found)

    for i, (start, size) in enumerate(slot_cuts):
        here = span(start, size)
        received(far_in.at[:, :, here], far_sem, i)
        gradients = []
        for b in range(blocks):
            total = paired[0, b, here].astype(jnp.float32)
            for j in range(1, far):
                total = total + far_in[j - 1, b, here].astype(jnp.float32)
            gradients.append(total.astype(jnp.bfloat16))
        for s in range(group):
            packed[s, here] = pick(block_of[s], gradients)
        for to in others:
            remote(
                packed.at[to, here],
                grad_turned.at[me_group, here],
                slot_sem,
                index_of(proj_cuts, start),
                group_id(to),
            ).start()

    for load in loads:
        load.wait()
    pltpu.make_async_copy(left, left, load_sem.at[3]).wait()
    first_part[...] = (beta_first / bias_first) * first[...].astype(jnp.float32)
    second_part[...] = (beta_second / bias_second) * second[...].astype(jnp.float32)

    def project(at, start, size):
        here = span(start, size)
        received(grad_turned.at[span(0, group - 1), here], slot_sem, at)
        grad_turned[me_group, here] = packed[me_group, here]
        lines = jnp.concatenate([grad_turned[s, here] for s in range(group)], axis=1)
        for to in partners + [me_dp]:
            result = jnp.dot(lines, left[to], preferred_element_type=jnp.float32).astype(
                jnp.bfloat16
            )
            if to is me_dp:
                proj_in[me_dp, here] = result
                continue
            proj_out[to, here] = result
            remote(
                proj_out.at[to, here], proj_in.at[me_dp, here], proj_sem, at, dp_id(to)
            ).start()

    def rotate(at, start, size, last):
        here = span(start, size)
        received(proj_in.at[span(0, replicas - 1), here], proj_sem, at)
        turned = jnp.concatenate([proj_in[e, here] for e in range(replicas)], axis=0).T
        for e in range(replicas):
            part = span(e * quarter, quarter)
            basis = jnp.concatenate(
                [right[span(d * quarter + start, size), part] for d in range(replicas)],
                axis=0,
            )
            rotated = jnp.dot(turned, basis, preferred_element_type=jnp.float32)
            if start > 0:
                rotated = rotated + partial[:, part]
            if not last:
                partial[:, part] = rotated
                continue
            first_new = first_part[:, part] + ((1.0 - beta_first) / bias_first) * rotated
            second_new = (
                second_part[:, part] + ((1.0 - beta_second) / bias_second) * rotated * rotated
            )
            direction[:, part] = (first_new / (jnp.sqrt(second_new) + epsilon)).astype(jnp.bfloat16)

    for i, (start, size) in enumerate(proj_cuts):
        project(i, start, size)
        if i == 1 and len(proj_cuts) > 2:
            rotate(0, *proj_cuts[0], False)
    for i, (start, size) in enumerate(proj_cuts):
        if i > 0 or len(proj_cuts) <= 2:
            rotate(i, start, size, i == len(proj_cuts) - 1)

    for at, (start, size) in enumerate(back_cuts):
        here = span(start, size)
        lines = jnp.concatenate(
            [
                right[pl.ds(pl.multiple_of(to * quarter + start, TILE_ROWS), size), :]
                for to in partners + [me_dp]
            ],
            axis=0,
        )
        result = lax.dot_general(
            lines, direction[...], (((1,), (1,)), ((), ())), preferred_element_type=jnp.float32
        ).astype(jnp.bfloat16)
        for i, to in enumerate(partners):
            back_out[i, here] = result[i * size : (i + 1) * size]
            remote(
                back_out.at[i, here], back_in.at[me_dp, here], back_sem, at, dp_id(to)
            ).start()
        back_in[me_dp, here] = result[len(partners) * size :]

    for at, (start, size) in enumerate(back_cuts):
        here = span(start, size)
        received(back_in.at[span(0, replicas - 1), here], back_sem, at)
        lines = [back_in[e, here] for e in range(replicas)]
        tile = middle * rows
        for h_at, side_at, across, h in tiles:
            first_to = h_at * owners + side_at * middle
            these = pl.ds(pl.multiple_of(first_to * rows, LANES), tile)
            total = lax.dot_general(
                lines[0], left[0, these], (((1,), (1,)), ((), ())), preferred_element_type=jnp.float32
            )
            for e in range(1, replicas):
                total = total + lax.dot_general(
                    lines[e],
                    left[e, these],
                    (((1,), (1,)), ((), ())),
                    preferred_element_type=jnp.float32,
                )
            result = total.astype(jnp.bfloat16)
            for i in range(middle):
                update[first_to + i, here] = result[:, i * rows : (i + 1) * rows]
            for i in range(middle - 1, -1, -1):
                if across or h or i:
                    to = first_to + (me_own + i) % middle
                    remote(
                        update.at[to, here],
                        returned.at[me_group, here],
                        return_sem,
                        at,
                        group_id(to),
                    ).start()

    filled = 0
    for at, (start, size) in enumerate(back_cuts):
        here = span(start, size)
        received(returned.at[span(0, group - 1), here], return_sem, at)
        returned[me_group, here] = update[me_group, here]
        arrived = [returned[s, here] for s in range(group)]
        for b in range(blocks):
            chosen[b, here] = pick(slots[b], arrived)
        while (filled + 1) * LANES <= start + size:
            for b in range(blocks):
                out[b, :, span(filled * LANES, LANES)] = chosen[b, span(filled * LANES, LANES)].T
            filled += 1

    sent(raw.at[1], near_sem)
    sent(far_in, far_sem)
    sent(packed.at[span(0, group - 1)], slot_sem)
    sent(proj_out.at[span(0, replicas - 1)], proj_sem)
    sent(back_out, back_sem)
    sent(update.at[span(0, group - 1)], return_sem)


def fused(grad_parts, owner_table, left_basis, right_basis, first_moment, second_moment):
    replicas, halves, owners = (lax.axis_size(a) for a in ("dp", "half", "own"))
    blocks, rows, width = grad_parts.shape[1:]
    quarter = width // replicas
    group = halves * owners
    far = replicas // 2
    lanes = quarter // LANES
    slot_cuts, proj_cuts, back_cuts = (cuts_of(quarter, c) for c in (SLOT_CUTS, PROJ_CUTS, BACK_CUTS))
    sizes = (replicas, halves, owners, blocks, rows, width, slot_cuts, proj_cuts, back_cuts)
    bf16, f32, dma = jnp.bfloat16, jnp.float32, pltpu.SemaphoreType.DMA
    hbm = pl.BlockSpec(memory_space=pl.ANY)
    return pl.pallas_call(
        functools.partial(step_kernel, sizes),
        out_shape=jax.ShapeDtypeStruct((blocks, rows, quarter), bf16),
        in_specs=[pl.BlockSpec(memory_space=pltpu.SMEM)] + [hbm] * 5,
        out_specs=pl.BlockSpec(memory_space=pltpu.VMEM),
        scratch_shapes=[
            pltpu.VMEM((2, far, lanes, blocks, rows, LANES), bf16),
            pltpu.VMEM((far, lanes, blocks, rows, LANES), bf16),
            pltpu.VMEM((far, blocks, quarter, rows), bf16),
            pltpu.VMEM((far - 1, blocks, quarter, rows), bf16),
            pltpu.VMEM((group, quarter, rows), bf16),
            pltpu.VMEM((group, quarter, rows), bf16),
            pltpu.VMEM((replicas, width, quarter), bf16),
            pltpu.VMEM((width, width), bf16),
            pltpu.VMEM((quarter, width), bf16),
            pltpu.VMEM((quarter, width), bf16),
            pltpu.VMEM((quarter, width), f32),
            pltpu.VMEM((quarter, width), f32),
            pltpu.VMEM((replicas, quarter, quarter), bf16),
            pltpu.VMEM((replicas, quarter, quarter), bf16),
            pltpu.VMEM((quarter, width), f32),
            pltpu.VMEM((quarter, width), bf16),
            pltpu.VMEM((replicas - 1, quarter, quarter), bf16),
            pltpu.VMEM((replicas, quarter, quarter), bf16),
            pltpu.VMEM((group, quarter, rows), bf16),
            pltpu.VMEM((group, quarter, rows), bf16),
            pltpu.VMEM((blocks, quarter, rows), bf16),
            dma((2, far, lanes)),
            dma((4,)),
            dma((1 + far * lanes,)),
            dma((1 + len(slot_cuts),)),
            dma((1 + len(proj_cuts),)),
            dma((1 + len(proj_cuts),)),
            dma((1 + len(back_cuts),)),
            dma((1 + len(back_cuts),)),
        ],
        compiler_params=pltpu.CompilerParams(collective_id=0, has_side_effects=True),
    )(owner_table.reshape(blocks), grad_parts.reshape(blocks, rows, width), left_basis, right_basis, first_moment, second_moment)


def cuts_of(quarter, parts):
    unit = quarter // sum(parts)
    return tuple((sum(parts[:i]) * unit, part * unit) for i, part in enumerate(parts))


def fits_kernel(mesh, rows, width):
    replicas = mesh.shape["dp"]
    return (
        replicas >= 4
        and replicas % 2 == 0
        and rows % LANES == 0
        and width % (replicas * LANES) == 0
    )


def route(mesh, *arrays):
    rows = arrays[0].shape[2]
    body = fused if fits_kernel(mesh, rows, arrays[0].shape[3]) else local
    return body(*arrays)


def solution(mesh):
    return jax.shard_map(
        functools.partial(route, mesh),
        mesh=mesh,
        in_specs=(
            P("dp", None, ("half", "own"), None),
            P(),
            P(("half", "own"), None, None),
            P(("half", "own"), None, None),
            P(("half", "own"), "dp", None),
            P(("half", "own"), "dp", None),
        ),
        out_specs=P(None, ("half", "own"), "dp"),
        check_vma=False,
    )
```

```python
import functools

import jax
import jax.numpy as jnp
from jax import lax
from jax.experimental import pallas as pl
from jax.experimental.pallas import tpu as pltpu
from jax.sharding import PartitionSpec as P

beta_first = 0.9
beta_second = 0.95
bias_first = 1.0 - 0.9**10
bias_second = 1.0 - 0.95**10
epsilon = 1e-08


def slot_select(owner_table, owner_count, slot_count):
    owner_ids = owner_table[:, 0]
    positions = jnp.arange(owner_ids.shape[0], dtype=jnp.int32)
    shared = (owner_ids[:, None] == owner_ids[None, :]) & (positions[None, :] < positions[:, None])
    ranking = jnp.sum(shared.astype(jnp.int32), axis=1)
    slot_ids = ranking * owner_count + owner_ids
    slot_range = jnp.arange(slot_count, dtype=jnp.int32)
    return (slot_range[:, None] == slot_ids[None, :]).astype(jnp.bfloat16)


def local(grad_parts, owner_table, left_basis, right_basis, first_moment, second_moment):
    halves = lax.axis_size("half")
    owners = lax.axis_size("own")
    replicas = lax.axis_size("dp")
    block_count = grad_parts.shape[1]
    piece_rows = grad_parts.shape[2]
    block_width = grad_parts.shape[3]
    quarter = block_width // replicas
    offset = lax.axis_index("dp") * quarter
    summed = lax.psum_scatter(
        grad_parts[0].astype(jnp.float32).astype(jnp.bfloat16),
        "dp",
        scatter_dimension=2,
        tiled=True,
    )
    selector = slot_select(owner_table, owners, halves * owners)
    flat_grad = summed.reshape(block_count, piece_rows * quarter)
    packed = jnp.dot(selector, flat_grad, preferred_element_type=jnp.float32).astype(jnp.bfloat16)
    packed = packed.reshape(halves, owners, piece_rows, quarter)
    arrived = lax.all_to_all(
        lax.all_to_all(packed, "half", split_axis=0, concat_axis=0, tiled=True),
        "own",
        split_axis=1,
        concat_axis=1,
        tiled=True,
    )
    grad_block = arrived.reshape(block_width, quarter)
    left_matrix = left_basis[0]
    right_matrix = right_basis[0]
    right_rows = lax.dynamic_slice_in_dim(right_matrix, offset, quarter, 0)
    left_slice = lax.dynamic_slice_in_dim(left_matrix, offset, quarter, 1)
    projected = lax.dot_general(
        left_slice,
        lax.all_gather(grad_block, "dp", axis=1, tiled=True),
        (((0,), (0,)), ((), ())),
        preferred_element_type=jnp.float32,
    )
    rotated = jnp.dot(
        projected.astype(jnp.bfloat16), right_matrix, preferred_element_type=jnp.float32
    )
    first_new = beta_first * first_moment[0].astype(jnp.float32) + (1.0 - beta_first) * rotated
    second_new = (
        beta_second * second_moment[0].astype(jnp.float32) + (1.0 - beta_second) * rotated * rotated
    )
    direction = (first_new / bias_first / (jnp.sqrt(second_new / bias_second) + epsilon)).astype(
        jnp.bfloat16
    )
    partial_cols = lax.dot_general(
        lax.all_gather(direction, "dp", axis=0, tiled=True),
        right_rows,
        (((1,), (1,)), ((), ())),
        preferred_element_type=jnp.float32,
    )
    update_block = jnp.dot(
        left_matrix, partial_cols.astype(jnp.bfloat16), preferred_element_type=jnp.float32
    )
    outgoing = update_block.astype(jnp.bfloat16).reshape(halves, owners, piece_rows, quarter)
    returned = lax.all_to_all(
        lax.all_to_all(outgoing, "half", split_axis=0, concat_axis=0, tiled=True),
        "own",
        split_axis=1,
        concat_axis=1,
        tiled=True,
    )
    flat_back = returned.reshape(halves * owners, piece_rows * quarter)
    placed = lax.dot_general(
        selector, flat_back, (((0,), (0,)), ((), ())), preferred_element_type=jnp.float32
    )
    return placed.astype(jnp.bfloat16).reshape(block_count, piece_rows, quarter)


MESH = pl.DeviceIdType.MESH
LANES = 128
TILE_ROWS = 16
SLOT_CUTS = (1, 1, 1, 1, 2, 2)
PROJ_CUTS = (4, 2, 2)
BACK_CUTS = (3, 7, 6)


def pick(index, values):
    chosen = values[0]
    for i in range(1, len(values)):
        chosen = lax.select_n(index == i, chosen, values[i])
    return chosen


def step_kernel(
    sizes,
    table,
    grad,
    left_in,
    right_in,
    first_in,
    second_in,
    out,
    raw,
    near,
    paired,
    far_in,
    packed,
    grad_turned,
    left,
    right,
    first,
    second,
    first_part,
    second_part,
    proj_out,
    proj_in,
    partial,
    direction,
    back_out,
    back_in,
    update,
    returned,
    chosen,
    raw_sem,
    load_sem,
    near_sem,
    far_sem,
    slot_sem,
    proj_sem,
    back_sem,
    return_sem,
):
    replicas, halves, owners, blocks, rows, width, slot_cuts, proj_cuts, back_cuts = sizes
    far = replicas // 2
    group = halves * owners
    quarter = width // replicas
    lanes = quarter // LANES
    me_dp = lax.axis_index("dp")
    me_group = lax.axis_index("half") * owners + lax.axis_index("own")
    me_far = me_dp // 2
    parity = me_dp % 2
    mate = me_far * 2 + 1 - parity

    middle = max(1, owners // 2)
    sides = owners // middle
    me_half, me_own = me_group // owners, me_group % owners
    side = me_own // middle
    tiles = []
    for across in range(sides - 1, -1, -1):
        for h in range(halves - 1, -1, -1):
            tiles.append(((me_half + h) % halves, (side + across) % sides, across, h))
    others = []
    for h_at, side_at, across, h in tiles:
        for i in range(middle - 1, -1, -1):
            if across or h or i:
                others.append(h_at * owners + side_at * middle + (me_own + i) % middle)

    partners = []
    for j in range(1, far):
        for c in range(2):
            partners.append(((me_far + j) % far) * 2 + (parity + c) % 2)
    partners.append(mate)

    def dp_id(index):
        return {"dp": index}

    def group_id(index):
        return {"half": index // owners, "own": index % owners}

    def remote(src, dst, sems, index, target):
        return pltpu.make_async_remote_copy(
            src_ref=src,
            dst_ref=dst,
            send_sem=sems.at[0],
            recv_sem=sems.at[1 + index],
            device_id=target,
            device_id_type=MESH,
        )

    def received(ref, sems, index):
        remote(ref, ref, sems, index, dp_id(mate)).wait_recv()

    def sent(ref, sems):
        remote(ref, ref, sems, 0, dp_id(mate)).wait_send()

    def span(start, size):
        return slice(start, start + size)

    def index_of(cuts, at):
        return [start <= at < start + size for start, size in cuts].index(True)

    order = list(range(1, far)) + [0]
    raw_loads = {}
    for j in order:
        for k in range(lanes):
            for s in (1, 0):
                index = ((me_far + j) % far) * 2 + (1 - parity if s else parity)
                start = pl.multiple_of(index * quarter + k * LANES, LANES)
                raw_loads[s, j, k] = pltpu.make_async_copy(
                    grad.at[:, :, pl.ds(start, LANES)], raw.at[s, j, k], raw_sem.at[s, j, k]
                )
                raw_loads[s, j, k].start()

    barrier = pltpu.get_barrier_semaphore()
    for j in range(1, replicas):
        pl.semaphore_signal(
            barrier, inc=1, device_id=dp_id((me_dp + j) % replicas), device_id_type=MESH
        )
    for t in range(1, group):
        pl.semaphore_signal(
            barrier, inc=1, device_id=group_id((me_group + t) % group), device_id_type=MESH
        )

    pl.semaphore_wait(barrier, replicas - 1 + group - 1)

    for j in order:
        for k in range(lanes):
            raw_loads[1, j, k].wait()
            remote(
                raw.at[1, j, k], near.at[j, k], near_sem, j * lanes + k, dp_id(mate)
            ).start()

    loads = [
        pltpu.make_async_copy(first_in.at[0], first, load_sem.at[0]),
        pltpu.make_async_copy(second_in.at[0], second, load_sem.at[1]),
        pltpu.make_async_copy(right_in.at[0], right, load_sem.at[2]),
    ]
    left_loads = [
        pltpu.make_async_copy(
            left_in.at[0, :, span(e * quarter, quarter)], left.at[e], load_sem.at[3]
        )
        for e in range(replicas)
    ]
    for load in left_loads + loads:
        load.start()

    for j in order:
        for k in range(lanes):
            raw_loads[0, j, k].wait()
            received(near.at[j, k], near_sem, j * lanes + k)
            for b in range(blocks):
                paired[j, b, span(k * LANES, LANES)] = (
                    (raw[0, j, k, b].astype(jnp.float32) + near[j, k, b].astype(jnp.float32))
                    .astype(jnp.bfloat16)
                    .T
                )
            if j == 0:
                continue
            for i, (start, size) in enumerate(slot_cuts):
                if k * LANES < start + size <= (k + 1) * LANES:
                    remote(
                        paired.at[j, :, span(start, size)],
                        far_in.at[j - 1, :, span(start, size)],
                        far_sem,
                        i,
                        dp_id(((me_far + j) % far) * 2 + parity),
                    ).start()

    def slot_of(b):
        owner = table[b]
        rank = lax.fori_loop(
            0, b, lambda c, n: n + jnp.where(table[c] == owner, 1, 0), jnp.int32(0)
        )
        return rank * owners + owner

    slots = [slot_of(b) for b in range(blocks)]
    block_of = []
    for s in range(group):
        found = jnp.int32(0)
        for b in range(blocks):
            found = jnp.where(slots[b] == s, jnp.int32(b), found)
        block_of.append(found)

    for i, (start, size) in enumerate(slot_cuts):
        here = span(start, size)
        received(far_in.at[:, :, here], far_sem, i)
        gradients = []
        for b in range(blocks):
            total = paired[0, b, here].astype(jnp.float32)
            for j in range(1, far):
                total = total + far_in[j - 1, b, here].astype(jnp.float32)
            gradients.append(total.astype(jnp.bfloat16))
        for s in range(group):
            packed[s, here] = pick(block_of[s], gradients)
        for to in others:
            remote(
                packed.at[to, here],
                grad_turned.at[me_group, here],
                slot_sem,
                index_of(proj_cuts, start),
                group_id(to),
            ).start()

    for load in loads:
        load.wait()
    pltpu.make_async_copy(left, left, load_sem.at[3]).wait()
    first_part[...] = (beta_first / bias_first) * first[...].astype(jnp.float32)
    second_part[...] = (beta_second / bias_second) * second[...].astype(jnp.float32)

    def project(at, start, size):
        here = span(start, size)
        received(grad_turned.at[span(0, group - 1), here], slot_sem, at)
        grad_turned[me_group, here] = packed[me_group, here]
        lines = jnp.concatenate([grad_turned[s, here] for s in range(group)], axis=1)
        for to in partners + [me_dp]:
            result = jnp.dot(lines, left[to], preferred_element_type=jnp.float32).astype(
                jnp.bfloat16
            )
            if to is me_dp:
                proj_in[me_dp, here] = result
                continue
            proj_out[to, here] = result
            remote(
                proj_out.at[to, here], proj_in.at[me_dp, here], proj_sem, at, dp_id(to)
            ).start()

    def rotate(at, start, size, last):
        here = span(start, size)
        received(proj_in.at[span(0, replicas - 1), here], proj_sem, at)
        turned = jnp.concatenate([proj_in[e, here] for e in range(replicas)], axis=0).T
        for e in range(replicas):
            part = span(e * quarter, quarter)
            basis = jnp.concatenate(
                [right[span(d * quarter + start, size), part] for d in range(replicas)],
                axis=0,
            )
            rotated = jnp.dot(turned, basis, preferred_element_type=jnp.float32)
            if start > 0:
                rotated = rotated + partial[:, part]
            if not last:
                partial[:, part] = rotated
                continue
            first_new = first_part[:, part] + ((1.0 - beta_first) / bias_first) * rotated
            second_new = (
                second_part[:, part] + ((1.0 - beta_second) / bias_second) * rotated * rotated
            )
            direction[:, part] = (first_new / (jnp.sqrt(second_new) + epsilon)).astype(jnp.bfloat16)

    for i, (start, size) in enumerate(proj_cuts):
        project(i, start, size)
    for i, (start, size) in enumerate(proj_cuts):
        rotate(i, start, size, i == len(proj_cuts) - 1)

    for at, (start, size) in enumerate(back_cuts):
        here = span(start, size)
        lines = jnp.concatenate(
            [
                right[pl.ds(pl.multiple_of(to * quarter + start, TILE_ROWS), size), :]
                for to in partners + [me_dp]
            ],
            axis=0,
        )
        result = lax.dot_general(
            lines, direction[...], (((1,), (1,)), ((), ())), preferred_element_type=jnp.float32
        ).astype(jnp.bfloat16)
        for i, to in enumerate(partners):
            back_out[i, here] = result[i * size : (i + 1) * size]
            remote(
                back_out.at[i, here], back_in.at[me_dp, here], back_sem, at, dp_id(to)
            ).start()
        back_in[me_dp, here] = result[len(partners) * size :]

    for at, (start, size) in enumerate(back_cuts):
        here = span(start, size)
        received(back_in.at[span(0, replicas - 1), here], back_sem, at)
        lines = [back_in[e, here] for e in range(replicas)]
        tile = middle * rows
        for h_at, side_at, across, h in tiles:
            first_to = h_at * owners + side_at * middle
            these = pl.ds(pl.multiple_of(first_to * rows, LANES), tile)
            total = lax.dot_general(
                lines[0], left[0, these], (((1,), (1,)), ((), ())), preferred_element_type=jnp.float32
            )
            for e in range(1, replicas):
                total = total + lax.dot_general(
                    lines[e],
                    left[e, these],
                    (((1,), (1,)), ((), ())),
                    preferred_element_type=jnp.float32,
                )
            result = total.astype(jnp.bfloat16)
            for i in range(middle):
                update[first_to + i, here] = result[:, i * rows : (i + 1) * rows]
            for i in range(middle - 1, -1, -1):
                if across or h or i:
                    to = first_to + (me_own + i) % middle
                    remote(
                        update.at[to, here],
                        returned.at[me_group, here],
                        return_sem,
                        at,
                        group_id(to),
                    ).start()

    filled = 0
    for at, (start, size) in enumerate(back_cuts):
        here = span(start, size)
        received(returned.at[span(0, group - 1), here], return_sem, at)
        returned[me_group, here] = update[me_group, here]
        arrived = [returned[s, here] for s in range(group)]
        for b in range(blocks):
            chosen[b, here] = pick(slots[b], arrived)
        while (filled + 1) * LANES <= start + size:
            for b in range(blocks):
                out[b, :, span(filled * LANES, LANES)] = chosen[b, span(filled * LANES, LANES)].T
            filled += 1

    sent(raw.at[1], near_sem)
    sent(far_in, far_sem)
    sent(packed.at[span(0, group - 1)], slot_sem)
    sent(proj_out.at[span(0, replicas - 1)], proj_sem)
    sent(back_out, back_sem)
    sent(update.at[span(0, group - 1)], return_sem)


def fused(grad_parts, owner_table, left_basis, right_basis, first_moment, second_moment):
    replicas, halves, owners = (lax.axis_size(a) for a in ("dp", "half", "own"))
    blocks, rows, width = grad_parts.shape[1:]
    quarter = width // replicas
    group = halves * owners
    far = replicas // 2
    lanes = quarter // LANES
    slot_cuts, proj_cuts, back_cuts = (cuts_of(quarter, c) for c in (SLOT_CUTS, PROJ_CUTS, BACK_CUTS))
    sizes = (replicas, halves, owners, blocks, rows, width, slot_cuts, proj_cuts, back_cuts)
    bf16, f32, dma = jnp.bfloat16, jnp.float32, pltpu.SemaphoreType.DMA
    hbm = pl.BlockSpec(memory_space=pl.ANY)
    return pl.pallas_call(
        functools.partial(step_kernel, sizes),
        out_shape=pltpu.VMEM((blocks, rows, quarter), bf16),
        in_specs=[pl.BlockSpec(memory_space=pltpu.SMEM)] + [hbm] * 5,
        out_specs=pl.BlockSpec(memory_space=pltpu.VMEM),
        scratch_shapes=[
            pltpu.VMEM((2, far, lanes, blocks, rows, LANES), bf16),
            pltpu.VMEM((far, lanes, blocks, rows, LANES), bf16),
            pltpu.VMEM((far, blocks, quarter, rows), bf16),
            pltpu.VMEM((far - 1, blocks, quarter, rows), bf16),
            pltpu.VMEM((group, quarter, rows), bf16),
            pltpu.VMEM((group, quarter, rows), bf16),
            pltpu.VMEM((replicas, width, quarter), bf16),
            pltpu.VMEM((width, width), bf16),
            pltpu.VMEM((quarter, width), bf16),
            pltpu.VMEM((quarter, width), bf16),
            pltpu.VMEM((quarter, width), f32),
            pltpu.VMEM((quarter, width), f32),
            pltpu.VMEM((replicas, quarter, quarter), bf16),
            pltpu.VMEM((replicas, quarter, quarter), bf16),
            pltpu.VMEM((quarter, width), f32),
            pltpu.VMEM((quarter, width), bf16),
            pltpu.VMEM((replicas - 1, quarter, quarter), bf16),
            pltpu.VMEM((replicas, quarter, quarter), bf16),
            pltpu.VMEM((group, quarter, rows), bf16),
            pltpu.VMEM((group, quarter, rows), bf16),
            pltpu.VMEM((blocks, quarter, rows), bf16),
            dma((2, far, lanes)),
            dma((4,)),
            dma((1 + far * lanes,)),
            dma((1 + len(slot_cuts),)),
            dma((1 + len(proj_cuts),)),
            dma((1 + len(proj_cuts),)),
            dma((1 + len(back_cuts),)),
            dma((1 + len(back_cuts),)),
        ],
        compiler_params=pltpu.CompilerParams(collective_id=0, has_side_effects=True),
    )(owner_table.reshape(blocks), grad_parts.reshape(blocks, rows, width), left_basis, right_basis, first_moment, second_moment)


def cuts_of(quarter, parts):
    unit = quarter // sum(parts)
    return tuple((sum(parts[:i]) * unit, part * unit) for i, part in enumerate(parts))


def fits_kernel(mesh, rows, width):
    replicas = mesh.shape["dp"]
    return (
        replicas >= 4
        and replicas % 2 == 0
        and rows % LANES == 0
        and width % (replicas * LANES) == 0
    )


def route(mesh, *arrays):
    rows = arrays[0].shape[2]
    body = fused if fits_kernel(mesh, rows, arrays[0].shape[3]) else local
    return body(*arrays)


def solution(mesh):
    return jax.shard_map(
        functools.partial(route, mesh),
        mesh=mesh,
        in_specs=(
            P("dp", None, ("half", "own"), None),
            P(),
            P(("half", "own"), None, None),
            P(("half", "own"), None, None),
            P(("half", "own"), "dp", None),
            P(("half", "own"), "dp", None),
        ),
        out_specs=P(None, ("half", "own"), "dp"),
        check_vma=False,
    )
```

```python
import functools

import jax
import jax.numpy as jnp
from jax import lax
from jax.experimental import pallas as pl
from jax.experimental.pallas import tpu as pltpu
from jax.sharding import PartitionSpec as P

beta_first = 0.9
beta_second = 0.95
bias_first = 1.0 - 0.9**10
bias_second = 1.0 - 0.95**10
epsilon = 1e-08


def slot_select(owner_table, owner_count, slot_count):
    owner_ids = owner_table[:, 0]
    positions = jnp.arange(owner_ids.shape[0], dtype=jnp.int32)
    shared = (owner_ids[:, None] == owner_ids[None, :]) & (positions[None, :] < positions[:, None])
    ranking = jnp.sum(shared.astype(jnp.int32), axis=1)
    slot_ids = ranking * owner_count + owner_ids
    slot_range = jnp.arange(slot_count, dtype=jnp.int32)
    return (slot_range[:, None] == slot_ids[None, :]).astype(jnp.bfloat16)


def local(grad_parts, owner_table, left_basis, right_basis, first_moment, second_moment):
    halves = lax.axis_size("half")
    owners = lax.axis_size("own")
    replicas = lax.axis_size("dp")
    block_count = grad_parts.shape[1]
    piece_rows = grad_parts.shape[2]
    block_width = grad_parts.shape[3]
    quarter = block_width // replicas
    offset = lax.axis_index("dp") * quarter
    summed = lax.psum_scatter(
        grad_parts[0].astype(jnp.float32).astype(jnp.bfloat16),
        "dp",
        scatter_dimension=2,
        tiled=True,
    )
    selector = slot_select(owner_table, owners, halves * owners)
    flat_grad = summed.reshape(block_count, piece_rows * quarter)
    packed = jnp.dot(selector, flat_grad, preferred_element_type=jnp.float32).astype(jnp.bfloat16)
    packed = packed.reshape(halves, owners, piece_rows, quarter)
    arrived = lax.all_to_all(
        lax.all_to_all(packed, "half", split_axis=0, concat_axis=0, tiled=True),
        "own",
        split_axis=1,
        concat_axis=1,
        tiled=True,
    )
    grad_block = arrived.reshape(block_width, quarter)
    left_matrix = left_basis[0]
    right_matrix = right_basis[0]
    right_rows = lax.dynamic_slice_in_dim(right_matrix, offset, quarter, 0)
    left_slice = lax.dynamic_slice_in_dim(left_matrix, offset, quarter, 1)
    projected = lax.dot_general(
        left_slice,
        lax.all_gather(grad_block, "dp", axis=1, tiled=True),
        (((0,), (0,)), ((), ())),
        preferred_element_type=jnp.float32,
    )
    rotated = jnp.dot(
        projected.astype(jnp.bfloat16), right_matrix, preferred_element_type=jnp.float32
    )
    first_new = beta_first * first_moment[0].astype(jnp.float32) + (1.0 - beta_first) * rotated
    second_new = (
        beta_second * second_moment[0].astype(jnp.float32) + (1.0 - beta_second) * rotated * rotated
    )
    direction = (first_new / bias_first / (jnp.sqrt(second_new / bias_second) + epsilon)).astype(
        jnp.bfloat16
    )
    partial_cols = lax.dot_general(
        lax.all_gather(direction, "dp", axis=0, tiled=True),
        right_rows,
        (((1,), (1,)), ((), ())),
        preferred_element_type=jnp.float32,
    )
    update_block = jnp.dot(
        left_matrix, partial_cols.astype(jnp.bfloat16), preferred_element_type=jnp.float32
    )
    outgoing = update_block.astype(jnp.bfloat16).reshape(halves, owners, piece_rows, quarter)
    returned = lax.all_to_all(
        lax.all_to_all(outgoing, "half", split_axis=0, concat_axis=0, tiled=True),
        "own",
        split_axis=1,
        concat_axis=1,
        tiled=True,
    )
    flat_back = returned.reshape(halves * owners, piece_rows * quarter)
    placed = lax.dot_general(
        selector, flat_back, (((0,), (0,)), ((), ())), preferred_element_type=jnp.float32
    )
    return placed.astype(jnp.bfloat16).reshape(block_count, piece_rows, quarter)


MESH = pl.DeviceIdType.MESH
LANES = 128
TILE_ROWS = 16
SLOT_CUTS = (1, 1, 2, 2, 2, 4, 4)
PROJ_CUTS = (4, 2, 2)
BACK_CUTS = (3, 7, 6)


def pick(index, values):
    chosen = values[0]
    for i in range(1, len(values)):
        chosen = lax.select_n(index == i, chosen, values[i])
    return chosen


def step_kernel(
    sizes,
    table,
    grad,
    left_in,
    right_in,
    first_in,
    second_in,
    out,
    raw,
    near,
    paired,
    far_in,
    packed,
    grad_turned,
    left,
    right,
    first,
    second,
    first_part,
    second_part,
    proj_out,
    proj_in,
    partial,
    direction,
    back_out,
    back_in,
    update,
    returned,
    chosen,
    raw_sem,
    load_sem,
    near_sem,
    far_sem,
    slot_sem,
    proj_sem,
    back_sem,
    return_sem,
):
    replicas, halves, owners, blocks, rows, width, slot_cuts, proj_cuts, back_cuts = sizes
    far = replicas // 2
    group = halves * owners
    quarter = width // replicas
    lanes = quarter // LANES
    me_dp = lax.axis_index("dp")
    me_group = lax.axis_index("half") * owners + lax.axis_index("own")
    me_far = me_dp // 2
    parity = me_dp % 2
    mate = me_far * 2 + 1 - parity

    middle = max(1, owners // 2)
    sides = owners // middle
    me_half, me_own = me_group // owners, me_group % owners
    side = me_own // middle
    tiles = []
    for across in range(sides - 1, -1, -1):
        for h in range(halves - 1, -1, -1):
            tiles.append(((me_half + h) % halves, (side + across) % sides, across, h))
    others = []
    for h_at, side_at, across, h in tiles:
        for i in range(middle - 1, -1, -1):
            if across or h or i:
                others.append(h_at * owners + side_at * middle + (me_own + i) % middle)

    partners = []
    for j in range(1, far):
        for c in range(2):
            partners.append(((me_far + j) % far) * 2 + (parity + c) % 2)
    partners.append(mate)

    def dp_id(index):
        return {"dp": index}

    def group_id(index):
        return {"half": index // owners, "own": index % owners}

    def remote(src, dst, sems, index, target):
        return pltpu.make_async_remote_copy(
            src_ref=src,
            dst_ref=dst,
            send_sem=sems.at[0],
            recv_sem=sems.at[1 + index],
            device_id=target,
            device_id_type=MESH,
        )

    def received(ref, sems, index):
        remote(ref, ref, sems, index, dp_id(mate)).wait_recv()

    def sent(ref, sems):
        remote(ref, ref, sems, 0, dp_id(mate)).wait_send()

    def span(start, size):
        return slice(start, start + size)

    def index_of(cuts, at):
        return [start <= at < start + size for start, size in cuts].index(True)

    barrier = pltpu.get_barrier_semaphore()
    for j in range(1, replicas):
        pl.semaphore_signal(
            barrier, inc=1, device_id=dp_id((me_dp + j) % replicas), device_id_type=MESH
        )
    for t in range(1, group):
        pl.semaphore_signal(
            barrier, inc=1, device_id=group_id((me_group + t) % group), device_id_type=MESH
        )

    order = list(range(1, far)) + [0]
    for j in order:
        for k in range(lanes):
            for s in (1, 0):
                index = ((me_far + j) % far) * 2 + (1 - parity if s else parity)
                start = pl.multiple_of(index * quarter + k * LANES, LANES)
                pltpu.make_async_copy(
                    grad.at[:, :, pl.ds(start, LANES)], raw.at[s, j, k], raw_sem.at[s, j]
                ).start()

    pl.semaphore_wait(barrier, replicas - 1 + group - 1)

    for j in order:
        for k in range(lanes):
            if k == 0:
                pltpu.make_async_copy(raw.at[1, j], raw.at[1, j], raw_sem.at[1, j]).wait()
            remote(
                raw.at[1, j, k], near.at[j, k], near_sem, j * lanes + k, dp_id(mate)
            ).start()

    loads = [
        pltpu.make_async_copy(first_in.at[0], first, load_sem.at[0]),
        pltpu.make_async_copy(second_in.at[0], second, load_sem.at[1]),
        pltpu.make_async_copy(right_in.at[0], right, load_sem.at[2]),
    ]
    left_loads = [
        pltpu.make_async_copy(
            left_in.at[0, :, span(e * quarter, quarter)], left.at[e], load_sem.at[3]
        )
        for e in range(replicas)
    ]
    for load in left_loads + loads:
        load.start()

    for j in order:
        for k in range(lanes):
            if k == 0:
                pltpu.make_async_copy(raw.at[0, j], raw.at[0, j], raw_sem.at[0, j]).wait()
            received(near.at[j, k], near_sem, j * lanes + k)
            for b in range(blocks):
                paired[j, b, span(k * LANES, LANES)] = (
                    (raw[0, j, k, b].astype(jnp.float32) + near[j, k, b].astype(jnp.float32))
                    .astype(jnp.bfloat16)
                    .T
                )
            if j == 0:
                continue
            for i, (start, size) in enumerate(slot_cuts):
                if k * LANES < start + size <= (k + 1) * LANES:
                    remote(
                        paired.at[j, :, span(start, size)],
                        far_in.at[j - 1, :, span(start, size)],
                        far_sem,
                        i,
                        dp_id(((me_far + j) % far) * 2 + parity),
                    ).start()

    def slot_of(b):
        owner = table[b]
        rank = lax.fori_loop(
            0, b, lambda c, n: n + jnp.where(table[c] == owner, 1, 0), jnp.int32(0)
        )
        return rank * owners + owner

    slots = [slot_of(b) for b in range(blocks)]
    block_of = []
    for s in range(group):
        found = jnp.int32(0)
        for b in range(blocks):
            found = jnp.where(slots[b] == s, jnp.int32(b), found)
        block_of.append(found)

    for i, (start, size) in enumerate(slot_cuts):
        here = span(start, size)
        received(far_in.at[:, :, here], far_sem, i)
        gradients = []
        for b in range(blocks):
            total = paired[0, b, here].astype(jnp.float32)
            for j in range(1, far):
                total = total + far_in[j - 1, b, here].astype(jnp.float32)
            gradients.append(total.astype(jnp.bfloat16))
        for s in range(group):
            packed[s, here] = pick(block_of[s], gradients)
        for to in others:
            remote(
                packed.at[to, here],
                grad_turned.at[me_group, here],
                slot_sem,
                index_of(proj_cuts, start),
                group_id(to),
            ).start()

    for load in loads:
        load.wait()
    pltpu.make_async_copy(left, left, load_sem.at[3]).wait()
    first_part[...] = (beta_first / bias_first) * first[...].astype(jnp.float32)
    second_part[...] = (beta_second / bias_second) * second[...].astype(jnp.float32)

    def project(at, start, size):
        here = span(start, size)
        received(grad_turned.at[span(0, group - 1), here], slot_sem, at)
        grad_turned[me_group, here] = packed[me_group, here]
        lines = jnp.concatenate([grad_turned[s, here] for s in range(group)], axis=1)
        for to in partners + [me_dp]:
            result = jnp.dot(lines, left[to], preferred_element_type=jnp.float32).astype(
                jnp.bfloat16
            )
            if to is me_dp:
                proj_in[me_dp, here] = result
                continue
            proj_out[to, here] = result
            remote(
                proj_out.at[to, here], proj_in.at[me_dp, here], proj_sem, at, dp_id(to)
            ).start()

    def rotate(at, start, size, last):
        here = span(start, size)
        received(proj_in.at[span(0, replicas - 1), here], proj_sem, at)
        turned = jnp.concatenate([proj_in[e, here] for e in range(replicas)], axis=0).T
        for e in range(replicas):
            part = span(e * quarter, quarter)
            basis = jnp.concatenate(
                [right[span(d * quarter + start, size), part] for d in range(replicas)],
                axis=0,
            )
            rotated = jnp.dot(turned, basis, preferred_element_type=jnp.float32)
            if start > 0:
                rotated = rotated + partial[:, part]
            if not last:
                partial[:, part] = rotated
                continue
            first_new = first_part[:, part] + ((1.0 - beta_first) / bias_first) * rotated
            second_new = (
                second_part[:, part] + ((1.0 - beta_second) / bias_second) * rotated * rotated
            )
            direction[:, part] = (first_new / (jnp.sqrt(second_new) + epsilon)).astype(jnp.bfloat16)

    for i, (start, size) in enumerate(proj_cuts):
        project(i, start, size)
    for i, (start, size) in enumerate(proj_cuts):
        rotate(i, start, size, i == len(proj_cuts) - 1)

    for at, (start, size) in enumerate(back_cuts):
        here = span(start, size)
        lines = jnp.concatenate(
            [
                right[pl.ds(pl.multiple_of(to * quarter + start, TILE_ROWS), size), :]
                for to in partners + [me_dp]
            ],
            axis=0,
        )
        result = lax.dot_general(
            lines, direction[...], (((1,), (1,)), ((), ())), preferred_element_type=jnp.float32
        ).astype(jnp.bfloat16)
        for i, to in enumerate(partners):
            back_out[i, here] = result[i * size : (i + 1) * size]
            remote(
                back_out.at[i, here], back_in.at[me_dp, here], back_sem, at, dp_id(to)
            ).start()
        back_in[me_dp, here] = result[len(partners) * size :]

    for at, (start, size) in enumerate(back_cuts):
        here = span(start, size)
        received(back_in.at[span(0, replicas - 1), here], back_sem, at)
        lines = [back_in[e, here] for e in range(replicas)]
        tile = middle * rows
        for h_at, side_at, across, h in tiles:
            first_to = h_at * owners + side_at * middle
            these = pl.ds(pl.multiple_of(first_to * rows, LANES), tile)
            total = lax.dot_general(
                lines[0], left[0, these], (((1,), (1,)), ((), ())), preferred_element_type=jnp.float32
            )
            for e in range(1, replicas):
                total = total + lax.dot_general(
                    lines[e],
                    left[e, these],
                    (((1,), (1,)), ((), ())),
                    preferred_element_type=jnp.float32,
                )
            result = total.astype(jnp.bfloat16)
            for i in range(middle):
                update[first_to + i, here] = result[:, i * rows : (i + 1) * rows]
            for i in range(middle - 1, -1, -1):
                if across or h or i:
                    to = first_to + (me_own + i) % middle
                    remote(
                        update.at[to, here],
                        returned.at[me_group, here],
                        return_sem,
                        at,
                        group_id(to),
                    ).start()

    filled = 0
    for at, (start, size) in enumerate(back_cuts):
        here = span(start, size)
        received(returned.at[span(0, group - 1), here], return_sem, at)
        returned[me_group, here] = update[me_group, here]
        arrived = [returned[s, here] for s in range(group)]
        for b in range(blocks):
            chosen[b, here] = pick(slots[b], arrived)
        while (filled + 1) * LANES <= start + size:
            for b in range(blocks):
                out[b, :, span(filled * LANES, LANES)] = chosen[b, span(filled * LANES, LANES)].T
            filled += 1

    sent(raw.at[1], near_sem)
    sent(far_in, far_sem)
    sent(packed.at[span(0, group - 1)], slot_sem)
    sent(proj_out.at[span(0, replicas - 1)], proj_sem)
    sent(back_out, back_sem)
    sent(update.at[span(0, group - 1)], return_sem)


def fused(grad_parts, owner_table, left_basis, right_basis, first_moment, second_moment):
    replicas, halves, owners = (lax.axis_size(a) for a in ("dp", "half", "own"))
    blocks, rows, width = grad_parts.shape[1:]
    quarter = width // replicas
    group = halves * owners
    far = replicas // 2
    lanes = quarter // LANES
    slot_cuts, proj_cuts, back_cuts = (cuts_of(quarter, c) for c in (SLOT_CUTS, PROJ_CUTS, BACK_CUTS))
    sizes = (replicas, halves, owners, blocks, rows, width, slot_cuts, proj_cuts, back_cuts)
    bf16, f32, dma = jnp.bfloat16, jnp.float32, pltpu.SemaphoreType.DMA
    hbm = pl.BlockSpec(memory_space=pl.ANY)
    return pl.pallas_call(
        functools.partial(step_kernel, sizes),
        out_shape=pltpu.VMEM((blocks, rows, quarter), bf16),
        in_specs=[pl.BlockSpec(memory_space=pltpu.SMEM)] + [hbm] * 5,
        out_specs=pl.BlockSpec(memory_space=pltpu.VMEM),
        scratch_shapes=[
            pltpu.VMEM((2, far, lanes, blocks, rows, LANES), bf16),
            pltpu.VMEM((far, lanes, blocks, rows, LANES), bf16),
            pltpu.VMEM((far, blocks, quarter, rows), bf16),
            pltpu.VMEM((far - 1, blocks, quarter, rows), bf16),
            pltpu.VMEM((group, quarter, rows), bf16),
            pltpu.VMEM((group, quarter, rows), bf16),
            pltpu.VMEM((replicas, width, quarter), bf16),
            pltpu.VMEM((width, width), bf16),
            pltpu.VMEM((quarter, width), bf16),
            pltpu.VMEM((quarter, width), bf16),
            pltpu.VMEM((quarter, width), f32),
            pltpu.VMEM((quarter, width), f32),
            pltpu.VMEM((replicas, quarter, quarter), bf16),
            pltpu.VMEM((replicas, quarter, quarter), bf16),
            pltpu.VMEM((quarter, width), f32),
            pltpu.VMEM((quarter, width), bf16),
            pltpu.VMEM((replicas - 1, quarter, quarter), bf16),
            pltpu.VMEM((replicas, quarter, quarter), bf16),
            pltpu.VMEM((group, quarter, rows), bf16),
            pltpu.VMEM((group, quarter, rows), bf16),
            pltpu.VMEM((blocks, quarter, rows), bf16),
            dma((2, far)),
            dma((4,)),
            dma((1 + far * lanes,)),
            dma((1 + len(slot_cuts),)),
            dma((1 + len(proj_cuts),)),
            dma((1 + len(proj_cuts),)),
            dma((1 + len(back_cuts),)),
            dma((1 + len(back_cuts),)),
        ],
        compiler_params=pltpu.CompilerParams(collective_id=0, has_side_effects=True),
    )(owner_table.reshape(blocks), grad_parts.reshape(blocks, rows, width), left_basis, right_basis, first_moment, second_moment)


def cuts_of(quarter, parts):
    unit = quarter // sum(parts)
    return tuple((sum(parts[:i]) * unit, part * unit) for i, part in enumerate(parts))


def fits_kernel(mesh, rows, width):
    replicas = mesh.shape["dp"]
    return (
        replicas >= 4
        and replicas % 2 == 0
        and rows % LANES == 0
        and width % (replicas * LANES) == 0
    )


def route(mesh, *arrays):
    rows = arrays[0].shape[2]
    body = fused if fits_kernel(mesh, rows, arrays[0].shape[3]) else local
    return body(*arrays)


def solution(mesh):
    return jax.shard_map(
        functools.partial(route, mesh),
        mesh=mesh,
        in_specs=(
            P("dp", None, ("half", "own"), None),
            P(),
            P(("half", "own"), None, None),
            P(("half", "own"), None, None),
            P(("half", "own"), "dp", None),
            P(("half", "own"), "dp", None),
        ),
        out_specs=P(None, ("half", "own"), "dp"),
        check_vma=False,
    )
```
